32 devices in a mesh: seq: 8 (over z, y), head: 4 (over x, core).
Axes of the slice: x: 2, y: 2, z: 4, core: 2. Of those that a mesh axis runs over, the one named last changes fastest.
Arguments:
- queries: float32 [16, 512, 384], P('head', 'seq'), may hold values from -300 to 300
- keys: float32 [16, 512, 384], P('head', 'seq'), may hold values from -8 to 8
- values: float32 [16, 512, 384], P('head', 'seq'), may hold values from -6 to 6
- out_grad: float32 [16, 512, 384], P('head', 'seq'), may hold values from -6 to 6
- out_weight: float32 [768, 768], P('head'), may hold values from -0.21875 to 0.21875
Outputs:
- query_grad: float32 [16, 512, 384], P('head', 'seq')
- key_grad: float32 [16, 512, 384], P('head', 'seq')
- value_grad: float32 [16, 512, 384], P('head', 'seq')
- weight_grad: float32 [768, 768], P('head')
The draws below stay inside these ranges and needn't reach their ends.
All inputs are finite; a program needn't handle non-finite values.
Results may differ from the reference program's by a relative error of at most 0.0003.
Values sent between devices are 32-bit elements; how exact they have to be, the bound alone decides.
No kernel may reach another device: no remote copies, remote signals or barrier semaphores. Data moves between devices by JAX's collectives and lax.ppermute only.
A program may use at most 64 MiB of HBM per device.

```python
import jax
import jax.numpy as jnp
from jax import lax

HEAD_NUMBER = 16
HD = 48
LOCAL = 256
DILATION_RATE = 16
WIDTH = 768
TOKENS = 4096
GROUP = 8
SEGMENT = 4096
N_SEQ = 8


def head_layout(tensor):
    return tensor.transpose(1, 0, 2).reshape(HEAD_NUMBER, TOKENS // 8, 8 * HD)


def drawn_pair(key):
    base_key = jax.random.fold_in(key, 17)
    query_key, key_key = jax.random.split(base_key, 2)
    query_draw = jax.random.truncated_normal(query_key, -4.0, 4.0, (TOKENS, HEAD_NUMBER, HD), jnp.float32)
    key_draw = jax.random.truncated_normal(key_key, -4.0, 4.0, (TOKENS, HEAD_NUMBER, HD), jnp.float32)
    return (head_layout(query_draw), head_layout(key_draw))


def draw_queries(key, part):
    return drawn_pair(key)[0]


def draw_keys(key, part):
    return drawn_pair(key)[1]


def levels(stream_key, shape, shards, smallest, high):
    gain = 1.0
    for position, shards_of in shards:
        heights = jax.random.uniform(jax.random.fold_in(jax.random.fold_in(stream_key, 6), position), (shards_of,), jnp.float32, smallest / len(shards), high / len(shards))
        gain = gain * jnp.repeat(jnp.exp(heights), shape[position] // shards_of).reshape((-1,) + (1,) * (len(shape) - 1 - position))
    return gain


def noise(rng, dims, scale, most, shards=(), kind=jnp.bfloat16):
    drawn = scale * jax.random.normal(rng, dims, jnp.float32)
    if shards:
        drawn = drawn * levels(rng, dims, shards, -0.22, 0.18)
    return jnp.clip(drawn, -most, most).astype(kind)


def setup_inputs(seed: int = 0) -> dict:
    key_of = jax.random.split(jax.random.key(seed), 6)
    queries = draw_queries(jax.random.fold_in(key_of[5], 71), 0)
    keys = draw_keys(jax.random.fold_in(key_of[5], 71), 0)
    values = noise(key_of[2], (HEAD_NUMBER, TOKENS // 8, 8 * HD), 1.0, 6.0, ((0, 4), (1, 8)), jnp.float32)
    out_grad = noise(key_of[3], (HEAD_NUMBER, TOKENS // 8, 8 * HD), 1.0, 6.0, ((0, 4), (1, 8)), jnp.float32)
    out_weight = noise(key_of[4], (WIDTH, WIDTH), WIDTH ** -0.5, 0.21875, ((0, 4),), jnp.float32)
    return dict(queries=queries, keys=keys, values=values, out_grad=out_grad, out_weight=out_weight)


HIGHEST = lax.Precision.HIGHEST

def to_rows(tensor):
    head_count = tensor.shape[0]
    shaped = tensor.reshape(head_count, -1, HD).transpose(1, 0, 2)
    return shaped.reshape(-1, head_count * HD)

def to_heads(tensor, head_count):
    shaped = tensor.reshape(-1, head_count, HD).transpose(1, 0, 2)
    return shaped.reshape(head_count, -1, 8 * HD)

def segment_attention(query_row_set, key_rows, value_rows, score_scale):
    scores = jnp.einsum('sqhd,skhd->shqk', query_row_set, key_rows, precision=HIGHEST) * score_scale
    row_max = lax.stop_gradient(lax.optimization_barrier(jnp.max(scores, axis=-1, keepdims=True)))
    exponent = jnp.exp(scores - row_max)
    totals = lax.optimization_barrier(jnp.sum(exponent, axis=-1, keepdims=True))
    mixed_values = jnp.einsum('shqk,skhd->sqhd', exponent / totals, value_rows, precision=HIGHEST)
    log_total = jnp.transpose((row_max + jnp.log(totals))[..., 0], (0, 2, 1))
    return (mixed_values, log_total)

def pick_rows(tensor, picking_mask):
    dilation = picking_mask.shape[0]
    shaped = tensor.reshape((tensor.shape[0] // dilation, dilation) + tensor.shape[1:])
    weights = picking_mask.reshape((1,) + picking_mask.shape + (1,) * (tensor.ndim - 2))
    return lax.optimization_barrier(jnp.sum(shaped * weights, axis=1))

def spread_rows(tensor, picking_mask):
    placed = picking_mask[None, :, :, None] * tensor[:, None]
    return placed.reshape((-1,) + tensor.shape[1:])

def forward(query_row_set, key_rows, value_rows, far_rows, picking_mask, score_scale):
    row_count, present_heads, head_dim = query_row_set.shape

    def blocks(tensor):
        return tensor.reshape(row_count // LOCAL, LOCAL, present_heads, head_dim)
    local_out, local_lse = segment_attention(blocks(query_row_set), blocks(key_rows), blocks(value_rows), score_scale)
    local_out = local_out.reshape(row_count, present_heads, head_dim)
    local_lse = local_lse.reshape(row_count, present_heads)
    chosen = pick_rows(query_row_set, picking_mask)
    far_keys = far_rows[0].reshape(-1, present_heads, head_dim)
    far_values = far_rows[1].reshape(-1, present_heads, head_dim)
    wide_out, wide_lse = segment_attention(chosen[None], far_keys[None], far_values[None], score_scale)
    local_chosen = pick_rows(local_out, picking_mask)
    lse_chosen = pick_rows(local_lse, picking_mask)
    branch_share = jax.nn.sigmoid(wide_lse[0] - lse_chosen)[..., None]
    change = branch_share * (wide_out[0] - local_chosen)
    return (local_out + spread_rows(change, picking_mask)).reshape(row_count, present_heads * head_dim)

def reference(queries, keys, values, out_grad, out_weight):
    queries = to_rows(queries)
    keys = to_rows(keys)
    values = to_rows(values)
    out_grad = to_rows(out_grad)
    score_scale = HD ** (-0.5)
    count_of_groups = N_SEQ // GROUP
    d_attn = jnp.dot(out_grad, out_weight.T, precision=HIGHEST, preferred_element_type=jnp.float32)

    def arrange(tensor):
        shaped = tensor.reshape(count_of_groups, SEGMENT, HEAD_NUMBER, HD).transpose(0, 2, 1, 3)
        return shaped.reshape(count_of_groups * HEAD_NUMBER, SEGMENT, 1, HD)
    shift_amounts = jnp.arange(count_of_groups * HEAD_NUMBER, dtype=jnp.int32) % HEAD_NUMBER % DILATION_RATE

    def one_item(item_tuple):
        query_row_set, key_rows, value_rows, grad_rows, shift_amount = item_tuple
        picking_mask = (jnp.arange(DILATION_RATE, dtype=jnp.int32)[:, None] == shift_amount).astype(query_row_set.dtype)

        def whole_pass(query_part, key_part, value_part):
            far_rows = jnp.stack([pick_rows(key_part, picking_mask), pick_rows(value_part, picking_mask)])
            far_rows = far_rows.reshape(2, -1, HD)
            return forward(query_part, key_part, value_part, far_rows, picking_mask, score_scale)
        attended, pull_back = jax.vjp(whole_pass, query_row_set, key_rows, value_rows)
        gradients = pull_back(grad_rows.reshape(SEGMENT, HD))
        return (attended,) + tuple(gradients)
    attended, query_grad, key_grad, value_grad = lax.map(one_item, (arrange(queries), arrange(keys), arrange(values), arrange(d_attn), shift_amounts))

    def restore(tensor):
        shaped = tensor.reshape(count_of_groups, HEAD_NUMBER, SEGMENT, HD).transpose(0, 2, 1, 3)
        return shaped.reshape(TOKENS, HEAD_NUMBER * HD)
    attended = restore(attended)
    weight_grad = jnp.dot(attended.T, out_grad, precision=HIGHEST, preferred_element_type=jnp.float32)
    return (to_heads(restore(query_grad), HEAD_NUMBER), to_heads(restore(key_grad), HEAD_NUMBER), to_heads(restore(value_grad), HEAD_NUMBER), weight_grad)
```

```python
import functools

import jax
import jax.numpy as jnp
from jax import lax
from jax.experimental import pallas as pl
from jax.experimental.pallas import tpu as pltpu
from jax.sharding import PartitionSpec as P

HD = 48
PACK = 8
LOCAL = 256
DILATION_RATE = 16
SPAN = 16
LROWS = LOCAL // PACK
LANES = 128
STEP = DILATION_RATE // PACK
SCALE = HD ** (-0.5)
HIGHEST = lax.Precision.HIGHEST
F32 = jnp.float32
BF16 = jnp.bfloat16

NN = (((1,), (0,)), ((), ()))
NT = (((1,), (1,)), ((), ()))
TN = (((0,), (0,)), ((), ()))


def split2(x):
    hi = x.astype(BF16)
    return hi, (x - hi.astype(F32)).astype(BF16)


def mm(a, b, dims):
    return lax.dot_general(a, b, dims, preferred_element_type=F32)


def dots(a, b, dims):
    return mm(a[0], b[0], dims) + (mm(a[0], b[1], dims) + mm(a[1], b[0], dims))


def dot3(a, b, dims):
    return dots(split2(a), split2(b), dims)


def dot6(a, b, dims):
    return lax.dot_general(a, b, dims, precision=HIGHEST, preferred_element_type=F32)


def head_offset(h, heads):
    shift = (lax.axis_index("head") * heads + h) % DILATION_RATE
    return shift % PACK, shift // PACK


def slab(x, j):
    return x[:, j * HD : (j + 1) * HD]


def pad(x):
    return jnp.concatenate([x, jnp.zeros((x.shape[0], LANES - x.shape[1]), x.dtype)], axis=1)


def pick_slab(x, col):
    acc = slab(x, 0)
    for j in range(1, PACK):
        acc = jnp.where(col == j, slab(x, j), acc)
    return acc


def pick_kernel(k_ref, v_ref, o_ref, tmp):
    heads, rows, _ = k_ref.shape
    picked = rows // STEP
    parts = []
    for i, ref in enumerate((k_ref, v_ref)):
        for h in range(heads):
            col, par = head_offset(h, heads)
            tmp[i * heads + h, :, :HD] = pick_slab(ref[h], col)
            x = tmp[i * heads + h, pl.ds(par, picked, stride=STEP), :]
            parts.append(x[:, :HD])
    o_ref[...] = jnp.concatenate(parts, axis=1)


def local_fwd_kernel(q_ref, k_ref, v_ref, qr, kr, vr, o_ref, p_ref):
    rows = q_ref.shape[1]
    for src, dst in ((q_ref, qr), (k_ref, kr), (v_ref, vr)):
        x = src[0]
        for j in range(PACK):
            dst[0, j, :, :HD] = slab(x, j)
    for g in range(rows // LROWS):
        sl = pl.ds(g * LROWS, LROWS)
        q, k, v = (r[0, :, sl, :].reshape(LOCAL, LANES)[:, :HD] for r in (qr, kr, vr))
        s = dot6(q, k, NT) * SCALE
        m = jnp.max(s, axis=1, keepdims=True)
        e = jnp.exp(s - m)
        l = jnp.sum(e, axis=1, keepdims=True)
        p = e * (1.0 / l)
        o = dot3(p, v, NN)
        p_ref[0, g] = p
        lse = m + jnp.log(l)
        both = jnp.concatenate([o, jnp.broadcast_to(lse, (LOCAL, LANES - HD))], axis=1)
        o_ref[0, :, sl, :] = both.reshape(PACK, LROWS, LANES)


def dattn_kernel(*refs):
    blocks = len(refs) - 4
    og = refs[:blocks]
    w_ref, hi_ref, lo_ref, da_ref = refs[blocks:]
    heads, rows, _ = og[0].shape
    cols = heads * HD
    me = lax.axis_index("head")
    for p in range(blocks):
        b = me ^ p
        for j in range(PACK):
            x = jnp.concatenate([slab(og[p][h], j) for h in range(heads)], axis=1)
            hi, lo = split2(x)
            hi_ref[b, j] = hi
            lo_ref[b, j] = lo
    acc = jnp.zeros((PACK * rows, cols), F32)
    for b in range(blocks):
        a = (hi_ref[b].reshape(PACK * rows, cols), lo_ref[b].reshape(PACK * rows, cols))
        acc = acc + dots(a, split2(w_ref[:, b * cols : (b + 1) * cols]), NT)
    for h in range(heads):
        da_ref[h, :, :, :HD] = slab(acc, h).reshape(PACK, rows, HD)


def far_kernel(*refs):
    n_in = len(refs) - 5
    kv = refs[: n_in - 5]
    qr, o_ref, da_ref, hi_ref, lo_ref = refs[n_in - 5 : n_in]
    wg_ref, far_ref, aux_ref, dqf_ref, attn = refs[n_in:]
    heads, _, rows, _ = qr.shape
    cols = heads * HD
    picked = rows // STEP
    kvs = jnp.concatenate([r[...] for r in kv], axis=0)
    aux_ref[...] = jnp.zeros_like(aux_ref)
    dks, dvs, attns = [], [], []
    for h in range(heads):
        col, par = head_offset(h, heads)
        at = (h, col, pl.ds(par, picked, stride=STEP), slice(None))
        q, ol, da = (r[at] for r in (qr, o_ref, da_ref))
        lsel = ol[:, HD : HD + 1]
        q, ol, da = (x[:, :HD] for x in (q, ol, da))
        k, v = slab(kvs, h), slab(kvs, heads + h)
        s = dot6(q, k, NT) * SCALE
        m = jnp.max(s, axis=1, keepdims=True)
        e = jnp.exp(s - m)
        l = jnp.sum(e, axis=1, keepdims=True)
        p = e * (1.0 / l)
        vs = split2(v)
        ps = split2(p)
        of = dots(ps, vs, NN)
        share = 1.0 / (1.0 + jnp.exp(lsel - (m + jnp.log(l))))
        diff = of - ol
        attn[h] = o_ref[h]
        attn[h, col, pl.ds(par, picked, stride=STEP), :] = pad(ol + share * diff)
        attns.append(attn[h].reshape(PACK * rows, LANES)[:, :HD])
        gl = jnp.sum(da * diff, axis=1, keepdims=True) * share * (1.0 - share)
        do = da * share
        dos = split2(do)
        dp = dots(dos, vs, NT)
        ds = p * (dp - jnp.sum(do * of, axis=1, keepdims=True) + gl) * SCALE
        dss = split2(ds)
        dqf_ref[h] = pad(dots(dss, split2(k), NN))
        dks.append(dots(dss, split2(q), TN))
        dvs.append(dots(ps, dos, TN))
        lane = lax.broadcasted_iota(jnp.int32, (picked, LANES), 1)
        aux_ref[at] = jnp.where(lane == 0, share, -gl)
    far_ref[...] = jnp.concatenate(dks + dvs, axis=1)
    a = split2(jnp.concatenate(attns, axis=1))
    for b in range(hi_ref.shape[0]):
        g = (hi_ref[b].reshape(PACK * rows, cols), lo_ref[b].reshape(PACK * rows, cols))
        wg_ref[:, b * cols : (b + 1) * cols] = dots(a, g, TN)


def local_bwd_kernel(
    p_ref, qr, kr, vr, o_ref, da_ref, aux_ref, dqf_ref, dq_ref, dk_ref, dv_ref, sq, sk, sv
):
    heads = pl.num_programs(0)
    rows = qr.shape[2]
    picked = rows // STEP
    for g in range(rows // LROWS):
        sl = pl.ds(g * LROWS, LROWS)
        q, k, v, o, da = (
            r[0, :, sl, :].reshape(LOCAL, LANES)[:, :HD] for r in (qr, kr, vr, o_ref, da_ref)
        )
        aux = aux_ref[0, :, sl, :].reshape(LOCAL, LANES)
        share, gl = aux[:, 0:1], aux[:, 1:2]
        do = da * (1.0 - share)
        p = p_ref[0, g]
        dos = split2(do)
        dp = dots(dos, split2(v), NT)
        ds = p * (dp - (jnp.sum(do * o, axis=1, keepdims=True) - gl)) * SCALE
        dss = split2(ds)
        for dst, val in (
            (sq, dots(dss, split2(k), NN)),
            (sk, dots(dss, split2(q), TN)),
            (sv, dots(split2(p), dos, TN)),
        ):
            dst[:, sl, :] = pad(val).reshape(PACK, LROWS, LANES)
    shift = (lax.axis_index("head") * heads + pl.program_id(0)) % DILATION_RATE
    at = (shift % PACK, pl.ds(shift // PACK, picked, stride=STEP), slice(None))
    sq[at] = sq[at] + dqf_ref[0]
    for src, dst in ((sq, dq_ref), (sk, dk_ref), (sv, dv_ref)):
        dst[0] = jnp.concatenate([src[j][:, :HD] for j in range(PACK)], axis=1)


def add_kernel(dk_in, dv_in, far_ref, dk_ref, dv_ref, tmp):
    heads, rows, _ = dk_in.shape
    picked = rows // STEP
    far = far_ref[...]
    tmp[...] = jnp.zeros_like(tmp)
    for i, (src, dst) in enumerate(((dk_in, dk_ref), (dv_in, dv_ref))):
        for h in range(heads):
            col, par = head_offset(h, heads)
            n = i * heads + h
            tmp[n, pl.ds(par, picked, stride=STEP), :] = pad(slab(far, n))
            x = tmp[n][:, :HD]
            zero = jnp.zeros_like(x)
            x = jnp.concatenate([jnp.where(col == j, x, zero) for j in range(PACK)], axis=1)
            dst[h] = src[h] + x


def vm():
    return pl.BlockSpec(memory_space=pltpu.VMEM)


def sds(*shape, dtype=F32):
    return jax.ShapeDtypeStruct(shape, dtype)


def cost(flops):
    return pl.CostEstimate(flops=flops, bytes_accessed=1 << 20, transcendentals=0)


def call(kernel, outs, n_in, scratch=(), flops=1 << 20, **kw):
    return pl.pallas_call(
        kernel,
        out_shape=outs,
        in_specs=[vm()] * n_in,
        out_specs=jax.tree.map(lambda _: vm(), outs),
        scratch_shapes=list(scratch),
        cost_estimate=cost(flops),
        **kw,
    )


def head_spec(shape):
    rest = (0,) * (len(shape) - 1)
    return pl.BlockSpec((1,) + tuple(shape[1:]), lambda h: (h,) + rest)


def swap(x, axis, bit):
    n = lax.axis_size(axis)
    return lax.ppermute(x, axis, [(i, i ^ bit) for i in range(n)])


def bits_of(n):
    return [1 << i for i in range(n.bit_length() - 1)]


def on_device(queries, keys, values, out_grad, out_weight):
    heads, rows, _ = queries.shape
    cols = heads * HD
    width = out_weight.shape[1]
    picked = rows // STEP
    seq_n = lax.axis_size("seq")
    head_n = lax.axis_size("head")
    group = min(SPAN, seq_n)
    me = lax.axis_index("seq")

    gathered = {0: out_grad}
    for bit in bits_of(head_n)[::-1]:
        for p in list(gathered):
            gathered[p ^ bit] = swap(gathered[p], "head", bit)
    og = [gathered[p] for p in range(head_n)]

    own = call(pick_kernel, sds(picked, 2 * cols), 2, [pltpu.VMEM((2 * heads, rows, LANES), F32)])(keys, values)
    parts = [own]
    for bit in bits_of(group)[::-1]:
        sent = parts[0] if len(parts) == 1 else jnp.concatenate(parts, axis=0)
        parts.append(swap(sent, "seq", bit))

    rel = sds(heads, PACK, rows, LANES)
    segs = rows // LROWS
    probs = sds(heads, segs, LOCAL, LOCAL)
    hs = lambda s: head_spec(s.shape)
    nat = sds(heads, rows, PACK * HD)
    qr, kr, vr, o_rel, p_all = pl.pallas_call(
        local_fwd_kernel,
        grid=(heads,),
        out_shape=(rel, rel, rel, rel, probs),
        in_specs=[hs(nat)] * 3,
        out_specs=tuple(hs(s) for s in (rel, rel, rel, rel, probs)),
        cost_estimate=cost(1 << 31),
    )(queries, keys, values)

    terms = sds(head_n, PACK, rows, cols, dtype=BF16)
    hi, lo, da = call(dattn_kernel, (terms, terms, rel), head_n + 1, flops=1 << 29)(
        *og, out_weight
    )

    wg, far, aux, dqf = call(
        far_kernel,
        (
            sds(cols, width),
            sds(group * picked, 2 * cols),
            rel,
            sds(heads, picked, LANES),
        ),
        len(parts) + 5,
        scratch=[pltpu.VMEM((heads, PACK, rows, LANES), F32)],
        flops=1 << 29,
    )(*parts, qr, o_rel, da, hi, lo)

    dq, dk, dv = pl.pallas_call(
        local_bwd_kernel,
        grid=(heads,),
        out_shape=(nat, nat, nat),
        in_specs=[hs(probs)] + [hs(rel)] * 6 + [head_spec(dqf.shape)],
        out_specs=(hs(nat),) * 3,
        scratch_shapes=[pltpu.VMEM((PACK, rows, LANES), F32)] * 3,
        cost_estimate=cost(1 << 32),
    )(p_all, qr, kr, vr, o_rel, da, aux, dqf)

    scatter, whole = [], []
    left = cols
    for bit in bits_of(seq_n):
        if left % 16 == 0:
            scatter.append(bit)
            left //= 2
        else:
            whole.append(bit)
    for bit in scatter:
        n = wg.shape[0] // 2
        up = (me // bit) % 2
        mine = lax.dynamic_slice_in_dim(wg, up * n, n, 0)
        other = lax.dynamic_slice_in_dim(wg, (1 - up) * n, n, 0)
        wg = mine + swap(other, "seq", bit)
    for bit in whole:
        wg = wg + swap(wg, "seq", bit)
    for bit in scatter[::-1]:
        up = (me // bit) % 2
        other = swap(wg, "seq", bit)
        wg = jnp.where(
            up == 0, jnp.concatenate([wg, other], 0), jnp.concatenate([other, wg], 0)
        )

    for bit in bits_of(group):
        n = far.shape[0] // 2
        far = far[:n] + swap(far[n:], "seq", bit)
    dk, dv = call(
        add_kernel,
        (nat, nat),
        3,
        [pltpu.VMEM((2 * heads, rows, LANES), F32)],
        1 << 22,
        input_output_aliases={0: 0, 1: 1},
    )(dk, dv, far)
    return dq, dk, dv, wg


def solution(mesh):
    spec = P("head", "seq", None)
    return jax.shard_map(
        on_device,
        mesh=mesh,
        in_specs=(spec,) * 4 + (P("head", None),),
        out_specs=(spec,) * 3 + (P("head", None),),
        check_vma=False,
    )
```
